32 devices in a mesh: gx: 4 (over x, core), gy: 8 (over z, y).
Axes of the slice: x: 2, y: 2, z: 4, core: 2. Of those that a mesh axis runs over, the one named last changes fastest.
Arguments:
- hot_ids: int32 [262144], P(('gx', 'gy')), may hold values from 0 to 2047
- hot_grads: bfloat16 [262144, 128], P(('gx', 'gy')), may hold values from -6 to 6
- cold_grads: bfloat16 [4, 8, 8, 512, 128], P('gx', 'gy'), may hold values from -6 to 6
- cold_slots: int32 [4, 8, 8, 512], P('gx', 'gy'), may hold values from 0 to 2047
- cold_counts: int32 [4, 8, 8], P('gx', 'gy'), may hold values from 1 to 512, as said below
Outputs:
- hot_grad: float32 [2048, 128], replicated
- cold_grad: float32 [4, 16384, 128], P('gx', 'gy')
The draws below stay inside these ranges and needn't reach their ends.
Inputs may be any that keep to these rules, and one draw needn't show every extreme that they name: In each group g, some owner d receives cold_counts[g, s, d] = 512 from every s; loads per owner are skewed.
All inputs are finite; a program needn't handle non-finite values.
Results may differ from the reference program's by a relative error of at most 0.0003.
Values may be sent and summed in bfloat16 or wider, within the bound.
A program may use at most 64 MiB of HBM per device.

```python
import jax
import jax.numpy as jnp
from jax import lax

D = 128
HOT = 2048
LOOK = 8192
CAP = 512
OWN_ROWS = 2048
LOOKUPS = 262144
N_GX = 4
N_GY = 8


def draw_cold_counts(key, part):
    first = jax.random.fold_in(key, 11)
    second = jax.random.fold_in(key, 12)
    third = jax.random.fold_in(key, 13)
    limits = jax.random.randint(first, (N_GX, 1, N_GY), 1, CAP + 1)
    counts = jax.random.randint(second, (N_GX, N_GY, N_GY), 1, CAP + 1)
    counts = jnp.minimum(counts, limits)
    heavy = jax.random.randint(third, (N_GX, 1, 1), 0, N_GY)
    owners = jnp.arange(N_GY, dtype=jnp.int32)[None, None, :]
    return jnp.where(owners == heavy, CAP, counts).astype(jnp.int32)


def with_ends(values, rng, least, high):
    dims = values.shape
    spot = [jax.random.randint(jax.random.fold_in(rng, axis), (), 0, dims[axis]) for axis in range(len(dims))]
    values = values.at[tuple(spot)].set(least)
    longest = dims.index(max(dims))
    spot[longest] = (spot[longest] + 1) % dims[longest]
    return values.at[tuple(spot)].set(high)


def block_levels(rng, dims, shards, low, top_value):
    def one(dim, blocks):
        steps = jax.random.uniform(jax.random.fold_in(jax.random.fold_in(rng, 6), dim), (blocks,), jnp.float32, low / len(shards), top_value / len(shards))
        return jnp.repeat(jnp.exp(steps), dims[dim] // blocks).reshape((-1,) + (1,) * (len(dims) - dim - 1))

    gain = one(*shards[0])
    for cut in shards[1:]:
        gain = gain * one(*cut)
    return gain


def scatter_about(own_key, shape, spread, bound, split=(), kind=jnp.bfloat16):
    gain = block_levels(own_key, shape, split, -0.22, 0.18) if split else 1.0
    result = jax.random.normal(own_key, shape, jnp.float32) * spread * gain
    return jnp.minimum(jnp.maximum(result, -bound), bound).astype(kind)


def setup_inputs(seed: int = 0) -> dict:
    arg_keys = jax.random.split(jax.random.key(seed), 6)
    hot_ids = with_ends(jax.random.randint(arg_keys[0], (LOOKUPS,), 0, HOT), jax.random.fold_in(arg_keys[0], 1), 0, HOT - 1).astype(jnp.int32)
    hot_grads = scatter_about(arg_keys[1], (LOOKUPS, D), 1.0, 6.0, ((0, 32),))
    cold_grads = scatter_about(arg_keys[2], (N_GX, N_GY, N_GY, CAP, D), 1.0, 6.0, ((0, 4), (1, 8)))
    cold_slots = with_ends(jax.random.randint(arg_keys[3], (N_GX, N_GY, N_GY, CAP), 0, OWN_ROWS), jax.random.fold_in(arg_keys[3], 1), 0, OWN_ROWS - 1).astype(jnp.int32)
    cold_counts = draw_cold_counts(jax.random.fold_in(arg_keys[5], 71), 0)
    return dict(hot_ids=hot_ids, hot_grads=hot_grads, cold_grads=cold_grads, cold_slots=cold_slots, cold_counts=cold_counts)


def reference(hot_ids, hot_grads, cold_grads, cold_slots, cold_counts):
    hot_sum = jax.ops.segment_sum(hot_grads.astype(jnp.float32), hot_ids, num_segments=HOT)
    hot_grad = hot_sum * (HOT / (LOOK * N_GX * N_GY)) ** 0.5
    places = jnp.arange(CAP, dtype=jnp.int32)
    valid = places[None, None, None, :] < cold_counts[..., None]
    payload = jnp.where(valid[..., None], cold_grads, jnp.zeros_like(cold_grads))
    owners = jnp.arange(N_GY, dtype=jnp.int32)[None, None, :, None] * OWN_ROWS
    table_rows = (owners + cold_slots).astype(jnp.int32)

    def one_group(pair):
        rows_data, rows_index = pair
        return jax.ops.segment_sum(rows_data.reshape(-1, D).astype(jnp.float32), rows_index.reshape(-1), num_segments=OWN_ROWS * N_GY)

    cold_grad = lax.map(one_group, (payload, table_rows))
    return hot_grad, cold_grad
```

```python
import functools

import jax
import jax.numpy as jnp
from jax import lax
from jax.experimental import pallas as pl
from jax.experimental.pallas import tpu as pltpu
from jax.sharding import PartitionSpec as P

HOT = 2048
OWN_ROWS = 2048
LANES = 128
HIGH = 4
MESH = pl.DeviceIdType.MESH


def add_block(acc, ids, data, pieces, low_rows):
    columns = ids.T
    lo_iota = lax.broadcasted_iota(jnp.int32, (low_rows, LANES), 0)
    selectors, rows = [], []
    for j in range(pieces):
        lo = jnp.bitwise_and(ids[j : j + 1, :], low_rows - 1)
        selectors.append(jnp.where(lo_iota == lo, 1.0, 0.0).astype(jnp.bfloat16))
        here = data[j * LANES : (j + 1) * LANES, :]
        column = jnp.broadcast_to(columns[:, j : j + 1], here.shape)
        parts = []
        for h in range(HIGH):
            inside = (column >= h * low_rows) & (column < (h + 1) * low_rows)
            parts.append(here * jnp.where(inside, 1.0, 0.0).astype(jnp.bfloat16))
        rows.append(jnp.concatenate(parts, axis=1))
    selector = jnp.concatenate(selectors, axis=1)
    spread = jnp.concatenate(rows, axis=0)
    acc[...] += jnp.dot(selector, spread, preferred_element_type=jnp.float32)


def kernel(
    nx, ny, factor, cap_pieces,
    ids_ref, hot_ref, slots_ref, cold_ref, hot_out, cold_out,
    acc, cacc, tab, full, crecv, srecv, r0, r1, r2, r3,
    csend, crsem, ssend, srsem, own_sem, hsend, hrecv,
):
    gx, gy = lax.axis_index("gx"), lax.axis_index("gy")
    px, py = 2 - nx % 2, 2 - ny % 2
    low_rows = HOT // HIGH
    own_low = OWN_ROWS // HIGH
    width = hot_ref.shape[1]

    stages = [
        (px, lax.rem(gx, px), lambda p: ((gx // px) * px + p, gy)),
        (nx // px, gx // px, lambda p: (p * px + lax.rem(gx, px), gy)),
        (py, lax.rem(gy, py), lambda p: (gx, (gy // py) * py + p)),
        (ny // py, gy // py, lambda p: (gx, p * py + lax.rem(gy, py))),
    ]
    barrier = pltpu.get_barrier_semaphore()
    greeted = 0
    for n, k, device in stages[:2]:
        for j in range(1, n):
            pl.semaphore_signal(barrier, inc=1, device_id=device(lax.rem(k + j, n)), device_id_type=MESH)
            greeted += 1
    for j in range(1, ny):
        pl.semaphore_signal(barrier, inc=1, device_id=(gx, lax.rem(gy + j, ny)), device_id_type=MESH)
        greeted += 1
    pl.semaphore_wait(barrier, greeted)

    def cold_copies(j):
        peer = lax.rem(gy + j, ny)
        return (
            pltpu.make_async_remote_copy(
                src_ref=cold_ref.at[peer], dst_ref=crecv.at[j],
                send_sem=csend.at[j], recv_sem=crsem.at[j],
                device_id=(gx, peer), device_id_type=MESH,
            ),
            pltpu.make_async_remote_copy(
                src_ref=slots_ref.at[peer], dst_ref=srecv.at[j],
                send_sem=ssend.at[j], recv_sem=srsem.at[j],
                device_id=(gx, peer), device_id_type=MESH,
            ),
        )

    for j in range(1, ny):
        for copy in cold_copies(j):
            copy.start()
    own = pltpu.make_async_copy(cold_ref.at[gy], crecv.at[0], own_sem)
    own.start()

    acc[...] = jnp.zeros_like(acc)
    cacc[...] = jnp.zeros_like(cacc)

    def hot_step(i, carry):
        pieces = ids_ref.shape[1]
        data = hot_ref[pl.ds(pl.multiple_of(i * pieces * LANES, LANES), pieces * LANES), :]
        add_block(acc, ids_ref[i], data, pieces, low_rows)
        return carry

    lax.fori_loop(0, ids_ref.shape[0], hot_step, 0)
    for h in range(HIGH):
        tab[h * low_rows : (h + 1) * low_rows, :] = acc[:, h * width : (h + 1) * width]

    base, size = 0, HOT
    used = 0
    regions = []
    for (n, k, device), landing in zip(stages, (r0, r1, r2, r3)):
        regions.append((base, size))
        sub = size // n
        copies = []
        for j in range(1, n):
            peer = lax.rem(k + j, n)
            copies.append(
                pltpu.make_async_remote_copy(
                    src_ref=tab.at[pl.ds(pl.multiple_of(base + peer * sub, 8), sub), :],
                    dst_ref=landing.at[j - 1],
                    send_sem=hsend.at[used], recv_sem=hrecv.at[used],
                    device_id=device(peer), device_id_type=MESH,
                )
            )
            used += 1
        for copy in copies:
            copy.start()
        for copy in copies:
            copy.wait()
        base, size = base + k * sub, sub
        if n > 1:
            rows = pl.ds(pl.multiple_of(base, 8), size)
            total = tab[rows, :]
            for j in range(1, n):
                total = total + landing[j - 1]
            tab[rows, :] = total

    rows = pl.ds(pl.multiple_of(base, 8), size)
    full[rows, :] = tab[rows, :] * factor

    def cold_all():
        own.wait()
        add_block(cacc, slots_ref[gy], crecv[0], cap_pieces, own_low)

        def cold_step(j, carry):
            for copy in cold_copies(j):
                copy.wait()
            add_block(cacc, srecv[j], crecv[j], cap_pieces, own_low)
            return carry

        lax.fori_loop(1, ny, cold_step, 0)
        for h in range(HIGH):
            cold_out[h * own_low : (h + 1) * own_low, :] = cacc[:, h * width : (h + 1) * width]

    for index in (3, 2, 1, 0):
        n, k, device = stages[index]
        copies = []
        for j in range(1, n):
            rows = pl.ds(pl.multiple_of(base, 8), size)
            copies.append(
                pltpu.make_async_remote_copy(
                    src_ref=full.at[rows, :], dst_ref=full.at[rows, :],
                    send_sem=hsend.at[used], recv_sem=hrecv.at[used],
                    device_id=device(lax.rem(k + j, n)), device_id_type=MESH,
                )
            )
            used += 1
        for copy in copies:
            copy.start()
        if index == 1:
            cold_all()
        for j, copy in enumerate(copies, 1):
            copy.wait_send()
            source = regions[index][0] + lax.rem(k - j + n, n) * size
            rows = pl.ds(pl.multiple_of(source, 8), size)
            pltpu.make_async_remote_copy(
                src_ref=full.at[rows, :], dst_ref=full.at[rows, :],
                send_sem=hsend.at[used - n + j], recv_sem=hrecv.at[used - n + j],
                device_id=device(lax.rem(k + j, n)), device_id_type=MESH,
            ).wait_recv()
        base, size = regions[index]
    hot_out[...] = full[...]


def per_device(nx, ny, hot_ids, hot_grads, cold_grads, cold_slots, cold_counts):
    look, width = hot_grads.shape
    owners, capacity = cold_slots.shape[2], cold_slots.shape[3]
    px, py = 2 - nx % 2, 2 - ny % 2
    factor = (HOT / (look * nx * ny)) ** 0.5
    places = lax.broadcasted_iota(jnp.int32, (owners, capacity), 1)
    slots = jnp.where(places < cold_counts.reshape(owners, 1), cold_slots.reshape(owners, capacity), -1)
    cap_pieces = capacity // LANES
    slots = slots.reshape(owners, cap_pieces, LANES)
    pad = -cap_pieces % 8
    slots = jnp.pad(slots, ((0, 0), (0, pad), (0, 0)), constant_values=-1)
    ids = hot_ids.reshape(-1, 8, LANES)
    s0 = HOT // px
    s1 = s0 // (nx // px)
    s2 = s1 // py
    s3 = s2 // (ny // py)
    n_hot = 2 * ((px - 1) + (nx // px - 1) + (py - 1) + (ny // py - 1))
    f32 = jnp.float32
    vmem = pl.BlockSpec(memory_space=pltpu.VMEM)
    hot, cold = pl.pallas_call(
        functools.partial(kernel, nx, ny, factor, cap_pieces),
        out_shape=(
            jax.ShapeDtypeStruct((HOT, width), f32),
            jax.ShapeDtypeStruct((OWN_ROWS, width), f32),
        ),
        in_specs=[vmem, vmem, vmem, pl.BlockSpec(memory_space=pl.ANY)],
        out_specs=(vmem, vmem),
        scratch_shapes=[
            pltpu.VMEM((HOT // HIGH, HIGH * width), f32),
            pltpu.VMEM((OWN_ROWS // HIGH, HIGH * width), f32),
            pltpu.VMEM((HOT, width), f32),
            pltpu.VMEM((HOT, width), f32),
            pltpu.VMEM((owners, capacity, width), jnp.bfloat16),
            pltpu.VMEM((owners, cap_pieces + pad, LANES), jnp.int32),
            pltpu.VMEM((max(px - 1, 1), s0, width), f32),
            pltpu.VMEM((max(nx // px - 1, 1), s1, width), f32),
            pltpu.VMEM((max(py - 1, 1), s2, width), f32),
            pltpu.VMEM((max(ny // py - 1, 1), s3, width), f32),
            pltpu.SemaphoreType.DMA((owners,)),
            pltpu.SemaphoreType.DMA((owners,)),
            pltpu.SemaphoreType.DMA((owners,)),
            pltpu.SemaphoreType.DMA((owners,)),
            pltpu.SemaphoreType.DMA,
            pltpu.SemaphoreType.DMA((n_hot,)),
            pltpu.SemaphoreType.DMA((n_hot,)),
        ],
        compiler_params=pltpu.CompilerParams(
            collective_id=0, has_side_effects=True, vmem_limit_bytes=32 * 1024 * 1024
        ),
    )(ids, hot_grads, slots, cold_grads.reshape(owners, capacity, width))
    return hot, cold.reshape(1, OWN_ROWS, width)


def solution(mesh):
    body = functools.partial(per_device, mesh.shape["gx"], mesh.shape["gy"])
    return jax.shard_map(
        body,
        mesh=mesh,
        in_specs=(
            P(("gx", "gy")),
            P(("gx", "gy"), None),
            P("gx", "gy", None, None, None),
            P("gx", "gy", None, None),
            P("gx", "gy", None),
        ),
        out_specs=(P(), P("gx", "gy", None)),
        check_vma=False,
    )
```

```python
import functools

import jax
import jax.numpy as jnp
from jax import lax
from jax.experimental import pallas as pl
from jax.experimental.pallas import tpu as pltpu
from jax.sharding import PartitionSpec as P

HOT = 2048
OWN_ROWS = 2048
LANES = 128
HIGH = 4
MESH = pl.DeviceIdType.MESH


def add_block(acc, ids, data, pieces, low_rows):
    columns = ids.T
    lo_iota = lax.broadcasted_iota(jnp.int32, (low_rows, LANES), 0)
    selectors, rows = [], []
    for j in range(pieces):
        lo = jnp.bitwise_and(ids[j : j + 1, :], low_rows - 1)
        selectors.append(jnp.where(lo_iota == lo, 1.0, 0.0).astype(jnp.bfloat16))
        here = data[j * LANES : (j + 1) * LANES, :]
        column = jnp.broadcast_to(columns[:, j : j + 1], here.shape)
        parts = []
        for h in range(HIGH):
            inside = (column >= h * low_rows) & (column < (h + 1) * low_rows)
            parts.append(here * jnp.where(inside, 1.0, 0.0).astype(jnp.bfloat16))
        rows.append(jnp.concatenate(parts, axis=1))
    selector = jnp.concatenate(selectors, axis=1)
    spread = jnp.concatenate(rows, axis=0)
    acc[...] += jnp.dot(selector, spread, preferred_element_type=jnp.float32)


def kernel(
    nx, ny, factor, cap_pieces,
    ids_ref, hot_ref, slots_ref, cold_ref, hot_out, cold_out,
    acc, cacc, tab, full, hotv, idsv, crecv, srecv, r0, a1, b1, a2, b2, a3, b3,
    csend, crsem, ssend, srsem, own_sem, hsend, hrecv,
):
    gx, gy = lax.axis_index("gx"), lax.axis_index("gy")
    px, py = 2 - nx % 2, 2 - ny % 2
    low_rows = HOT // HIGH
    own_low = OWN_ROWS // HIGH
    width = hot_ref.shape[1]
    landing_refs = (a1, b1, a2, b2, a3, b3)

    core = (px, lax.rem(gx, px), lambda p: ((gx // px) * px + p, gy))
    along_x = (nx // px, gx // px, lambda p: (p * px + lax.rem(gx, px), gy))
    pair_y = (py, lax.rem(gy, py), lambda p: (gx, (gy // py) * py + p))
    rest_y = (ny // py, gy // py, lambda p: (gx, p * py + lax.rem(gy, py)))
    chains = [[along_x, pair_y, rest_y], [pair_y, along_x, rest_y]]

    hot_copy = pltpu.make_async_copy(hot_ref, hotv, own_sem.at[1])
    ids_copy = pltpu.make_async_copy(ids_ref, idsv, own_sem.at[2])
    own = pltpu.make_async_copy(cold_ref.at[gy], crecv.at[0], own_sem.at[0])
    ids_copy.start()
    hot_copy.start()

    barrier = pltpu.get_barrier_semaphore()
    greeted = 0
    for n, k, device in (core, along_x):
        for j in range(1, n):
            pl.semaphore_signal(barrier, inc=1, device_id=device(lax.rem(k + j, n)), device_id_type=MESH)
            greeted += 1
    for j in range(1, ny):
        pl.semaphore_signal(barrier, inc=1, device_id=(gx, lax.rem(gy + j, ny)), device_id_type=MESH)
        greeted += 1
    pl.semaphore_wait(barrier, greeted)

    def cold_copies(j):
        peer = lax.rem(gy + j, ny)
        return (
            pltpu.make_async_remote_copy(
                src_ref=cold_ref.at[peer], dst_ref=crecv.at[j],
                send_sem=csend.at[j], recv_sem=crsem.at[j],
                device_id=(gx, peer), device_id_type=MESH,
            ),
            pltpu.make_async_remote_copy(
                src_ref=slots_ref.at[peer], dst_ref=srecv.at[j],
                send_sem=ssend.at[j], recv_sem=srsem.at[j],
                device_id=(gx, peer), device_id_type=MESH,
            ),
        )

    middle = ny // 2
    for j in range(1, ny):
        if j != middle:
            for copy in cold_copies(j):
                copy.start()
    own.start()

    acc[...] = jnp.zeros_like(acc)
    cacc[...] = jnp.zeros_like(cacc)
    ids_copy.wait()
    hot_copy.wait()

    def hot_step(i, carry):
        pieces = idsv.shape[1]
        data = hotv[pl.ds(pl.multiple_of(i * pieces * LANES, LANES), pieces * LANES), :]
        add_block(acc, idsv[i], data, pieces, low_rows)
        return carry

    lax.fori_loop(0, idsv.shape[0], hot_step, 0)
    for h in range(HIGH):
        tab[h * low_rows : (h + 1) * low_rows, :] = acc[:, h * width : (h + 1) * width]

    used = 0

    def scatter_start(stage, base, size, landing):
        nonlocal used
        n, k, device = stage
        sub = size // n
        copies = []
        for j in range(1, n):
            peer = lax.rem(k + j, n)
            copies.append(
                pltpu.make_async_remote_copy(
                    src_ref=tab.at[pl.ds(pl.multiple_of(base + peer * sub, 8), sub), :],
                    dst_ref=landing.at[j - 1],
                    send_sem=hsend.at[used], recv_sem=hrecv.at[used],
                    device_id=device(peer), device_id_type=MESH,
                )
            )
            copies[-1].start()
            used += 1
        return copies

    def scatter_end(copies, stage, base, size, landing):
        n, k, device = stage
        for copy in copies:
            copy.wait()
        sub = size // n
        base = base + k * sub
        if n > 1:
            rows = pl.ds(pl.multiple_of(base, 8), sub)
            total = tab[rows, :]
            for j in range(1, n):
                total = total + landing[j - 1]
            tab[rows, :] = total
        return base, sub

    def gather_start(stage, base, size):
        nonlocal used
        n, k, device = stage
        rows = pl.ds(pl.multiple_of(base, 8), size)
        first = used
        for j in range(1, n):
            pltpu.make_async_remote_copy(
                src_ref=full.at[rows, :], dst_ref=full.at[rows, :],
                send_sem=hsend.at[used], recv_sem=hrecv.at[used],
                device_id=device(lax.rem(k + j, n)), device_id_type=MESH,
            ).start()
            used += 1
        return first

    def gather_end(first, stage, base, size):
        n, k, device = stage
        for j in range(1, n):
            mine = pl.ds(pl.multiple_of(base, 8), size)
            theirs = pl.ds(pl.multiple_of(base + (lax.rem(k - j + n, n) - k) * size, 8), size)
            for rows, receive in ((mine, False), (theirs, True)):
                copy = pltpu.make_async_remote_copy(
                    src_ref=full.at[rows, :], dst_ref=full.at[rows, :],
                    send_sem=hsend.at[first + j - 1], recv_sem=hrecv.at[first + j - 1],
                    device_id=device(lax.rem(k + j, n)), device_id_type=MESH,
                )
                if receive:
                    copy.wait_recv()
                else:
                    copy.wait_send()

    def cold_range(start, stop):
        def cold_step(j, carry):
            for copy in cold_copies(j):
                copy.wait()
            add_block(cacc, srecv[j], crecv[j], cap_pieces, own_low)
            return carry

        lax.fori_loop(start, stop, cold_step, 0)

    copies = scatter_start(core, 0, HOT, r0)
    own.wait()
    add_block(cacc, slots_ref[gy], crecv[0], cap_pieces, own_low)
    base, size = scatter_end(copies, core, 0, HOT, r0)
    top = (base, size)
    half = size // 2
    places = [(base, half), (base + half, half)]
    history = []
    for step in range(3):
        landings = [landing_refs[2 * step], landing_refs[2 * step + 1]]
        history.append(list(places))
        pending = [
            scatter_start(chains[c][step], *places[c], landings[c]) for c in range(2)
        ]
        if step == 1:
            cold_range(1, middle // 2 + 1)
        if step == 2:
            cold_range(middle // 2 + 1, middle)
        places = [
            scatter_end(pending[c], chains[c][step], *places[c], landings[c]) for c in range(2)
        ]
    for place, size in places:
        rows = pl.ds(pl.multiple_of(place, 8), size)
        full[rows, :] = tab[rows, :] * factor
    for step in (2, 1, 0):
        firsts = [gather_start(chains[c][step], *places[c]) for c in range(2)]
        split = min(middle + middle // 2 + 1, ny)
        if step == 1:
            for copy in cold_copies(middle):
                copy.start()
            cold_range(middle + 1, split)
        if step == 0:
            cold_range(split, ny)
        for c in range(2):
            gather_end(firsts[c], chains[c][step], *places[c])
        places = history[step]
    first = gather_start(core, *top)
    cold_range(middle, middle + 1)
    for h in range(HIGH):
        cold_out[h * own_low : (h + 1) * own_low, :] = cacc[:, h * width : (h + 1) * width]
    gather_end(first, core, *top)
    hot_out[...] = full[...]


def per_device(nx, ny, hot_ids, hot_grads, cold_grads, cold_slots, cold_counts):
    look, width = hot_grads.shape
    owners, capacity = cold_slots.shape[2], cold_slots.shape[3]
    px, py = 2 - nx % 2, 2 - ny % 2
    factor = (HOT / (look * nx * ny)) ** 0.5
    places = lax.broadcasted_iota(jnp.int32, (owners, capacity), 1)
    slots = jnp.where(places < cold_counts.reshape(owners, 1), cold_slots.reshape(owners, capacity), -1)
    cap_pieces = capacity // LANES
    slots = slots.reshape(owners, cap_pieces, LANES)
    pad = -cap_pieces % 8
    slots = jnp.pad(slots, ((0, 0), (0, pad), (0, 0)), constant_values=-1)
    ids = hot_ids.reshape(-1, 8, LANES)
    nxr, nyr = nx // px, ny // py
    s0 = HOT // px
    half = s0 // 2
    n_hot = 2 * ((px - 1) + 2 * ((nxr - 1) + (py - 1) + (nyr - 1)))

    def landing(n, rows):
        return pltpu.VMEM((max(n - 1, 1), rows // n, width), f32)

    f32 = jnp.float32
    hbm = pl.BlockSpec(memory_space=pltpu.HBM)
    vmem = pl.BlockSpec(memory_space=pltpu.VMEM)
    hot, cold = pl.pallas_call(
        functools.partial(kernel, nx, ny, factor, cap_pieces),
        out_shape=(
            jax.ShapeDtypeStruct((HOT, width), f32),
            jax.ShapeDtypeStruct((OWN_ROWS, width), f32),
        ),
        in_specs=[hbm, hbm, vmem, hbm],
        out_specs=(vmem, vmem),
        scratch_shapes=[
            pltpu.VMEM((HOT // HIGH, HIGH * width), f32),
            pltpu.VMEM((OWN_ROWS // HIGH, HIGH * width), f32),
            pltpu.VMEM((HOT, width), f32),
            pltpu.VMEM((HOT, width), f32),
            pltpu.VMEM((look, width), jnp.bfloat16),
            pltpu.VMEM(ids.shape, jnp.int32),
            pltpu.VMEM((owners, capacity, width), jnp.bfloat16),
            pltpu.VMEM((owners, cap_pieces + pad, LANES), jnp.int32),
            landing(px, HOT),
            landing(nxr, half),
            landing(py, half),
            landing(py, half // nxr),
            landing(nxr, half // py),
            landing(nyr, half // nxr // py),
            landing(nyr, half // nxr // py),
            pltpu.SemaphoreType.DMA((owners,)),
            pltpu.SemaphoreType.DMA((owners,)),
            pltpu.SemaphoreType.DMA((owners,)),
            pltpu.SemaphoreType.DMA((owners,)),
            pltpu.SemaphoreType.DMA((3,)),
            pltpu.SemaphoreType.DMA((n_hot,)),
            pltpu.SemaphoreType.DMA((n_hot,)),
        ],
        compiler_params=pltpu.CompilerParams(
            collective_id=0, has_side_effects=True, vmem_limit_bytes=63 * 1024 * 1024 - 1536 * 1024
        ),
    )(ids, hot_grads, slots, cold_grads.reshape(owners, capacity, width))
    return hot, cold.reshape(1, OWN_ROWS, width)


def solution(mesh):
    body = functools.partial(per_device, mesh.shape["gx"], mesh.shape["gy"])
    return jax.shard_map(
        body,
        mesh=mesh,
        in_specs=(
            P(("gx", "gy")),
            P(("gx", "gy"), None),
            P("gx", "gy", None, None, None),
            P("gx", "gy", None, None),
            P("gx", "gy", None),
        ),
        out_specs=(P(), P("gx", "gy", None)),
        check_vma=False,
    )
```

```python
import functools

import jax
import jax.numpy as jnp
from jax import lax
from jax.experimental import pallas as pl
from jax.experimental.pallas import tpu as pltpu
from jax.sharding import PartitionSpec as P

HOT = 2048
OWN_ROWS = 2048
LANES = 128
HIGH = 4
MESH = pl.DeviceIdType.MESH


def add_block(acc, ids, data, pieces, low_rows):
    columns = ids.T
    lo_iota = lax.broadcasted_iota(jnp.int32, (low_rows, LANES), 0)
    selectors, rows = [], []
    for j in range(pieces):
        lo = jnp.bitwise_and(ids[j : j + 1, :], low_rows - 1)
        selectors.append(jnp.where(lo_iota == lo, 1.0, 0.0).astype(jnp.bfloat16))
        here = data[j * LANES : (j + 1) * LANES, :]
        column = jnp.broadcast_to(columns[:, j : j + 1], here.shape)
        parts = []
        for h in range(HIGH):
            inside = (column >= h * low_rows) & (column < (h + 1) * low_rows)
            parts.append(here * jnp.where(inside, 1.0, 0.0).astype(jnp.bfloat16))
        rows.append(jnp.concatenate(parts, axis=1))
    selector = jnp.concatenate(selectors, axis=1)
    spread = jnp.concatenate(rows, axis=0)
    acc[...] += jnp.dot(selector, spread, preferred_element_type=jnp.float32)


def kernel(
    nx, ny, factor, cap_pieces,
    ids_ref, hot_ref, slots_ref, cold_ref, hot_out, cold_out,
    acc, cacc, tab, full, hotv, idsv, crecv, srecv, r0, a1, b1, a2, b2, a3, b3,
    csend, crsem, ssend, srsem, own_sem, hsend, hrecv,
):
    gx, gy = lax.axis_index("gx"), lax.axis_index("gy")
    px, py = 2 - nx % 2, 2 - ny % 2
    low_rows = HOT // HIGH
    own_low = OWN_ROWS // HIGH
    width = hot_ref.shape[1]
    landing_refs = (a1, b1, a2, b2, a3, b3)

    core = (px, lax.rem(gx, px), lambda p: ((gx // px) * px + p, gy))
    along_x = (nx // px, gx // px, lambda p: (p * px + lax.rem(gx, px), gy))
    pair_y = (py, lax.rem(gy, py), lambda p: (gx, (gy // py) * py + p))
    rest_y = (ny // py, gy // py, lambda p: (gx, p * py + lax.rem(gy, py)))
    chains = [[along_x, pair_y, rest_y], [pair_y, along_x, rest_y]]

    hot_copy = pltpu.make_async_copy(hot_ref, hotv, own_sem.at[1])
    ids_copy = pltpu.make_async_copy(ids_ref, idsv, own_sem.at[2])
    own = pltpu.make_async_copy(cold_ref.at[gy], crecv.at[0], own_sem.at[0])
    ids_copy.start()
    hot_copy.start()

    barrier = pltpu.get_barrier_semaphore()
    greeted = 0
    for n, k, device in (core, along_x):
        for j in range(1, n):
            pl.semaphore_signal(barrier, inc=1, device_id=device(lax.rem(k + j, n)), device_id_type=MESH)
            greeted += 1
    for j in range(1, ny):
        pl.semaphore_signal(barrier, inc=1, device_id=(gx, lax.rem(gy + j, ny)), device_id_type=MESH)
        greeted += 1
    pl.semaphore_wait(barrier, greeted)

    def cold_copies(j):
        peer = lax.rem(gy + j, ny)
        return (
            pltpu.make_async_remote_copy(
                src_ref=cold_ref.at[peer], dst_ref=crecv.at[j],
                send_sem=csend.at[j], recv_sem=crsem.at[j],
                device_id=(gx, peer), device_id_type=MESH,
            ),
            pltpu.make_async_remote_copy(
                src_ref=slots_ref.at[peer], dst_ref=srecv.at[j],
                send_sem=ssend.at[j], recv_sem=srsem.at[j],
                device_id=(gx, peer), device_id_type=MESH,
            ),
        )

    middle = ny // 2
    for j in range(1, ny):
        if j != middle:
            for copy in cold_copies(j):
                copy.start()
    own.start()

    acc[...] = jnp.zeros_like(acc)
    cacc[...] = jnp.zeros_like(cacc)
    ids_copy.wait()
    hot_copy.wait()

    def hot_step(i, carry):
        pieces = idsv.shape[1]
        data = hotv[pl.ds(pl.multiple_of(i * pieces * LANES, LANES), pieces * LANES), :]
        add_block(acc, idsv[i], data, pieces, low_rows)
        return carry

    lax.fori_loop(0, idsv.shape[0], hot_step, 0)
    for h in range(HIGH):
        tab[h * low_rows : (h + 1) * low_rows, :] = acc[:, h * width : (h + 1) * width]

    used = 0

    def scatter_start(stage, base, size, landing):
        nonlocal used
        n, k, device = stage
        sub = size // n
        copies = []
        for j in range(1, n):
            peer = lax.rem(k + j, n)
            copies.append(
                pltpu.make_async_remote_copy(
                    src_ref=tab.at[pl.ds(pl.multiple_of(base + peer * sub, 8), sub), :],
                    dst_ref=landing.at[j - 1],
                    send_sem=hsend.at[used], recv_sem=hrecv.at[used],
                    device_id=device(peer), device_id_type=MESH,
                )
            )
            copies[-1].start()
            used += 1
        return copies

    def scatter_end(copies, stage, base, size, landing):
        n, k, device = stage
        for copy in copies:
            copy.wait()
        sub = size // n
        base = base + k * sub
        if n > 1:
            rows = pl.ds(pl.multiple_of(base, 8), sub)
            total = tab[rows, :]
            for j in range(1, n):
                total = total + landing[j - 1]
            tab[rows, :] = total
        return base, sub

    def gather_start(stage, base, size):
        nonlocal used
        n, k, device = stage
        rows = pl.ds(pl.multiple_of(base, 8), size)
        first = used
        for j in range(1, n):
            pltpu.make_async_remote_copy(
                src_ref=full.at[rows, :], dst_ref=full.at[rows, :],
                send_sem=hsend.at[used], recv_sem=hrecv.at[used],
                device_id=device(lax.rem(k + j, n)), device_id_type=MESH,
            ).start()
            used += 1
        return first

    def gather_end(first, stage, base, size):
        n, k, device = stage
        for j in range(1, n):
            mine = pl.ds(pl.multiple_of(base, 8), size)
            theirs = pl.ds(pl.multiple_of(base + (lax.rem(k - j + n, n) - k) * size, 8), size)
            for rows, receive in ((mine, False), (theirs, True)):
                copy = pltpu.make_async_remote_copy(
                    src_ref=full.at[rows, :], dst_ref=full.at[rows, :],
                    send_sem=hsend.at[first + j - 1], recv_sem=hrecv.at[first + j - 1],
                    device_id=device(lax.rem(k + j, n)), device_id_type=MESH,
                )
                if receive:
                    copy.wait_recv()
                else:
                    copy.wait_send()

    def cold_range(start, stop):
        def cold_step(j, carry):
            for copy in cold_copies(j):
                copy.wait()
            add_block(cacc, srecv[j], crecv[j], cap_pieces, own_low)
            return carry

        lax.fori_loop(start, stop, cold_step, 0)

    copies = scatter_start(core, 0, HOT, r0)
    own.wait()
    add_block(cacc, slots_ref[gy], crecv[0], cap_pieces, own_low)
    base, size = scatter_end(copies, core, 0, HOT, r0)
    top = (base, size)
    half = size // 2
    places = [(base, half), (base + half, half)]
    history = []
    for step in range(3):
        landings = [landing_refs[2 * step], landing_refs[2 * step + 1]]
        history.append(list(places))
        pending = [
            scatter_start(chains[c][step], *places[c], landings[c]) for c in range(2)
        ]
        places = [
            scatter_end(pending[c], chains[c][step], *places[c], landings[c]) for c in range(2)
        ]
    for place, size in places:
        rows = pl.ds(pl.multiple_of(place, 8), size)
        full[rows, :] = tab[rows, :] * factor
    for step in (2, 1, 0):
        firsts = [gather_start(chains[c][step], *places[c]) for c in range(2)]
        if step == 1:
            for copy in cold_copies(middle):
                copy.start()
            cold_range(1, middle)
        if step == 0:
            cold_range(middle + 1, ny)
        for c in range(2):
            gather_end(firsts[c], chains[c][step], *places[c])
        places = history[step]
    first = gather_start(core, *top)
    cold_range(middle, middle + 1)
    for h in range(HIGH):
        cold_out[h * own_low : (h + 1) * own_low, :] = cacc[:, h * width : (h + 1) * width]
    gather_end(first, core, *top)
    hot_out[...] = full[...]


def per_device(nx, ny, hot_ids, hot_grads, cold_grads, cold_slots, cold_counts):
    look, width = hot_grads.shape
    owners, capacity = cold_slots.shape[2], cold_slots.shape[3]
    px, py = 2 - nx % 2, 2 - ny % 2
    factor = (HOT / (look * nx * ny)) ** 0.5
    places = lax.broadcasted_iota(jnp.int32, (owners, capacity), 1)
    slots = jnp.where(places < cold_counts.reshape(owners, 1), cold_slots.reshape(owners, capacity), -1)
    cap_pieces = capacity // LANES
    slots = slots.reshape(owners, cap_pieces, LANES)
    pad = -cap_pieces % 8
    slots = jnp.pad(slots, ((0, 0), (0, pad), (0, 0)), constant_values=-1)
    ids = hot_ids.reshape(-1, 8, LANES)
    nxr, nyr = nx // px, ny // py
    s0 = HOT // px
    half = s0 // 2
    n_hot = 2 * ((px - 1) + 2 * ((nxr - 1) + (py - 1) + (nyr - 1)))

    def landing(n, rows):
        return pltpu.VMEM((max(n - 1, 1), rows // n, width), f32)

    f32 = jnp.float32
    hbm = pl.BlockSpec(memory_space=pltpu.HBM)
    vmem = pl.BlockSpec(memory_space=pltpu.VMEM)
    hot, cold = pl.pallas_call(
        functools.partial(kernel, nx, ny, factor, cap_pieces),
        out_shape=(
            jax.ShapeDtypeStruct((HOT, width), f32),
            jax.ShapeDtypeStruct((OWN_ROWS, width), f32),
        ),
        in_specs=[hbm, hbm, vmem, hbm],
        out_specs=(vmem, vmem),
        scratch_shapes=[
            pltpu.VMEM((HOT // HIGH, HIGH * width), f32),
            pltpu.VMEM((OWN_ROWS // HIGH, HIGH * width), f32),
            pltpu.VMEM((HOT, width), f32),
            pltpu.VMEM((HOT, width), f32),
            pltpu.VMEM((look, width), jnp.bfloat16),
            pltpu.VMEM(ids.shape, jnp.int32),
            pltpu.VMEM((owners, capacity, width), jnp.bfloat16),
            pltpu.VMEM((owners, cap_pieces + pad, LANES), jnp.int32),
            landing(px, HOT),
            landing(nxr, half),
            landing(py, half),
            landing(py, half // nxr),
            landing(nxr, half // py),
            landing(nyr, half // nxr // py),
            landing(nyr, half // nxr // py),
            pltpu.SemaphoreType.DMA((owners,)),
            pltpu.SemaphoreType.DMA((owners,)),
            pltpu.SemaphoreType.DMA((owners,)),
            pltpu.SemaphoreType.DMA((owners,)),
            pltpu.SemaphoreType.DMA((3,)),
            pltpu.SemaphoreType.DMA((n_hot,)),
            pltpu.SemaphoreType.DMA((n_hot,)),
        ],
        compiler_params=pltpu.CompilerParams(
            collective_id=0, has_side_effects=True, vmem_limit_bytes=63 * 1024 * 1024 - 1536 * 1024
        ),
    )(ids, hot_grads, slots, cold_grads.reshape(owners, capacity, width))
    return hot, cold.reshape(1, OWN_ROWS, width)


def solution(mesh):
    body = functools.partial(per_device, mesh.shape["gx"], mesh.shape["gy"])
    return jax.shard_map(
        body,
        mesh=mesh,
        in_specs=(
            P(("gx", "gy")),
            P(("gx", "gy"), None),
            P("gx", "gy", None, None, None),
            P("gx", "gy", None, None),
            P("gx", "gy", None),
        ),
        out_specs=(P(), P("gx", "gy", None)),
        check_vma=False,
    )
```
